32 devices in a mesh: row: 8 (over z, y), col: 4 (over x, core).
Axes of the slice: x: 2, y: 2, z: 4, core: 2. Of those that a mesh axis runs over, the one named last changes fastest.
Arguments:
- layer_input: bfloat16 [2048, 8192], P('row'), may hold values from -7 to 7
- gain: float32 [8192], replicated, may hold values from 0.5 to 6
- d_query: bfloat16 [2048, 4096], P('row', 'col'), may hold values from -6 to 6
- d_keyval: bfloat16 [2048, 2048], P('row', 'col'), may hold values from -6 to 6
- w_query: bfloat16 [8192, 4096], P('row', 'col'), may hold values from -0.0625 to 0.0625
- w_keyval: bfloat16 [8192, 2048], P('row', 'col'), may hold values from -1 to 1
- d_resid: bfloat16 [2048, 8192], P('row', 'col'), may hold values from -6 to 6
Outputs:
- d_input: bfloat16 [2048, 8192], P('row', 'col')
- grad_wq: bfloat16 [8192, 4096], P('row', 'col')
- grad_wkv: bfloat16 [8192, 2048], P('row', 'col')
- grad_gain: float32 [8192], P('col')
- grad_square_sum: float32 [], replicated
The draws below stay inside these ranges and needn't reach their ends.
All inputs are finite; a program needn't handle non-finite values.
Results may differ from the reference program's by a relative error of at most 0.023.
Values may be sent and summed in bfloat16 or wider, within the bound.
A program may use at most 128 MiB of HBM per device.

```python
import jax
import jax.numpy as jnp
from jax import lax

D = 8192
TOK_DEV = 256
QW = 4096
KVW = 2048
TOKENS = 2048
N_ROW = 8
N_COL = 4


def input_values(key):
    input_key = jax.random.fold_in(key, 101)
    return jnp.clip(jax.random.normal(input_key, (TOKENS, D), jnp.float32), -6.0, 6.0)


def keyval_values(key):
    weight_key = jax.random.fold_in(key, 202)
    factor = jnp.float32(1.0) / jnp.sqrt(jnp.float32(D))
    return jnp.clip(jax.random.normal(weight_key, (D, KVW), jnp.float32), -6.0, 6.0) * factor


def draw_layer_input(key, part):
    return input_values(key).astype(jnp.bfloat16)


def draw_gain(key, part):
    gain_key = jax.random.fold_in(key, 404)
    position = jnp.arange(D, dtype=jnp.float32) / jnp.float32(max(D - 1, 1))
    ramp = 1.0 + 2.0 * position
    factor = jax.random.uniform(gain_key, (D,), jnp.float32, 0.85, 1.15)
    return ramp * factor


def draw_w_keyval(key, part):
    return keyval_values(key).astype(jnp.bfloat16)


def draw_d_keyval(key, part):
    inputs = input_values(key)
    weights = keyval_values(key)
    scaled = inputs * lax.rsqrt(jnp.mean(inputs * inputs, axis=1, keepdims=True) + 1e-05)
    projected = jnp.dot(scaled, weights, precision=lax.Precision.HIGHEST)
    noise_key = jax.random.fold_in(key, 303)
    noise = jax.random.normal(noise_key, (TOKENS, KVW), jnp.float32)
    return jnp.clip(0.6 * projected + 0.8 * noise, -6.0, 6.0).astype(jnp.bfloat16)


def levels(own_key, shape, cuts, smallest, largest):
    def one(axis_at, blocks):
        heights = jax.random.uniform(jax.random.fold_in(jax.random.fold_in(own_key, 6), axis_at), (blocks,), jnp.float32, smallest / len(cuts), largest / len(cuts))
        return jnp.repeat(jnp.exp(heights), shape[axis_at] // blocks).reshape((-1,) + (1,) * (len(shape) - axis_at - 1))

    loudness = one(*cuts[0])
    for cut in cuts[1:]:
        loudness = loudness * one(*cut)
    return loudness


def bell_draw(rng, extent, deviation, bound, cuts=(), kind=jnp.bfloat16):
    entries = jax.random.normal(rng, extent, jnp.float32) * deviation
    if len(cuts) > 0:
        entries = levels(rng, extent, cuts, -0.22, 0.18) * entries
    return jnp.clip(entries, min=-bound, max=bound).astype(kind)


def setup_inputs(seed: int = 0) -> dict:
    arg_keys = jax.random.split(jax.random.key(seed), 8)
    layer_input = draw_layer_input(jax.random.fold_in(arg_keys[7], 71), 0)
    gain = draw_gain(jax.random.fold_in(arg_keys[7], 71), 0)
    d_query = bell_draw(arg_keys[2], (TOKENS, QW), 1.0, 6.0, ((0, 8), (1, 4)))
    d_keyval = draw_d_keyval(jax.random.fold_in(arg_keys[7], 71), 0)
    w_query = bell_draw(arg_keys[4], (D, QW), D ** -0.5, 0.0625, ((0, 8), (1, 4)))
    w_keyval = draw_w_keyval(jax.random.fold_in(arg_keys[7], 71), 0)
    d_resid = bell_draw(arg_keys[6], (TOKENS, D), 1.0, 6.0, ((0, 8), (1, 4)))
    return dict(layer_input=layer_input, gain=gain, d_query=d_query, d_keyval=d_keyval, w_query=w_query, w_keyval=w_keyval, d_resid=d_resid)


epsilon = 1e-05

def reference(layer_input, gain, d_query, d_keyval, w_query, w_keyval, d_resid):
    inputs = layer_input.astype(jnp.float32)
    inv_rms = lax.rsqrt(lax.optimization_barrier(jnp.mean(inputs * inputs, axis=1, keepdims=True)) + epsilon)
    normed = (inputs * inv_rms * gain).astype(jnp.bfloat16)
    query_cols = QW // N_COL
    keyval_cols = KVW // N_COL
    contract_cols = (((1,), (1,)), ((), ()))

    def add_block(block, accum_grad):
        qstart = (block * query_cols).astype(jnp.int32)
        kstart = (block * keyval_cols).astype(jnp.int32)
        qgrad = lax.dynamic_slice_in_dim(d_query, qstart, query_cols, 1)
        qweight = lax.dynamic_slice_in_dim(w_query, qstart, query_cols, 1)
        kgrad = lax.dynamic_slice_in_dim(d_keyval, kstart, keyval_cols, 1)
        kweight = lax.dynamic_slice_in_dim(w_keyval, kstart, keyval_cols, 1)
        partial_value = lax.dot_general(qgrad, qweight, contract_cols, preferred_element_type=jnp.float32)
        partial_value = partial_value + lax.dot_general(kgrad, kweight, contract_cols, preferred_element_type=jnp.float32)
        return accum_grad + partial_value.astype(jnp.bfloat16).astype(jnp.float32)
    feature_grad = lax.fori_loop(0, N_COL, add_block, jnp.zeros((TOKENS, D), jnp.float32))
    token_dot = lax.optimization_barrier(jnp.sum(gain * feature_grad * inputs, axis=1, keepdims=True))
    d_input = (d_resid.astype(jnp.float32) + inv_rms * gain * feature_grad - inputs * inv_rms ** 3 * token_dot / D).astype(jnp.bfloat16)
    scaling = 1.0 / jnp.sqrt(jnp.float32(TOKENS))
    grad_gain = lax.optimization_barrier(jnp.sum(feature_grad * inputs * inv_rms, axis=0)) * scaling
    weight_scale = 1.0 / jnp.sqrt(jnp.float32(TOK_DEV))
    contract_rows = (((0,), (0,)), ((), ()))

    def add_tokens(block, accums):
        tstart = (block * TOK_DEV).astype(jnp.int32)
        slab = lax.dynamic_slice_in_dim(normed, tstart, TOK_DEV, 0)
        qgrad = lax.dynamic_slice_in_dim(d_query, tstart, TOK_DEV, 0)
        kgrad = lax.dynamic_slice_in_dim(d_keyval, tstart, TOK_DEV, 0)
        block_q = lax.dot_general(slab, qgrad, contract_rows, preferred_element_type=jnp.float32) * weight_scale
        block_kv = lax.dot_general(slab, kgrad, contract_rows, preferred_element_type=jnp.float32) * weight_scale
        return (accums[0] + block_q.astype(jnp.bfloat16).astype(jnp.float32), accums[1] + block_kv.astype(jnp.bfloat16).astype(jnp.float32))
    sum_q, sum_kv = lax.fori_loop(0, N_ROW, add_tokens, (jnp.zeros((D, QW), jnp.float32), jnp.zeros((D, KVW), jnp.float32)))
    grad_wq = sum_q.astype(jnp.bfloat16)
    grad_wkv = sum_kv.astype(jnp.bfloat16)
    query_f = grad_wq.astype(jnp.float32)
    keyval_f = grad_wkv.astype(jnp.float32)
    grand_total = jnp.sum(query_f * query_f) + jnp.sum(keyval_f * keyval_f) + jnp.sum(grad_gain * grad_gain)
    grad_square_sum = grand_total / jnp.float32(D)
    return (d_input, grad_wq, grad_wkv, grad_gain, grad_square_sum)
```

```python
import math

import jax
import jax.numpy as jnp
from jax import lax
from jax.sharding import PartitionSpec as P

epsilon = 1e-05


def local(layer_input, gain, d_query, d_keyval, w_query, w_keyval, d_resid):
    inputs = layer_input.astype(jnp.float32)
    inv_rms = lax.rsqrt(jnp.mean(inputs * inputs, axis=1, keepdims=True) + epsilon)
    normed = (inputs * inv_rms * gain).astype(jnp.bfloat16)
    model_width = inputs.shape[1]
    local_tokens = inputs.shape[0]
    tokens_all = local_tokens * lax.axis_size("row")
    scaling = 1.0 / math.sqrt(tokens_all)
    weight_scale = 1.0 / math.sqrt(local_tokens)
    contract_cols = (((1,), (1,)), ((), ()))
    query_cols = d_query.shape[1]
    cotangent = jnp.concatenate([d_query, d_keyval], axis=1)
    all_cotangents = lax.all_gather(cotangent, "row", axis=0, tiled=True)
    weights = jnp.concatenate([w_query, w_keyval], axis=1)
    partial_value = lax.dot_general(
        all_cotangents, weights, contract_cols, preferred_element_type=jnp.float32
    )
    reduced = lax.psum_scatter(
        partial_value.astype(jnp.bfloat16), "col", scatter_dimension=0, tiled=True
    )
    n_row, n_col = lax.axis_size("row"), lax.axis_size("col")
    fold = n_row // n_col
    pieces = reduced.reshape(fold, local_tokens, reduced.shape[1])
    row, col = lax.axis_index("row"), lax.axis_index("col")
    arrived = []
    for shift in range(fold):
        pairs = [
            (r * n_col + c, (fold * c + (r + shift) % fold) * n_col + r // fold)
            for r in range(n_row)
            for c in range(n_col)
        ]
        piece = lax.dynamic_index_in_dim(pieces, (row + shift) % fold, 0, keepdims=False)
        arrived.append(lax.ppermute(piece, ("row", "col"), pairs))
    arrived = jnp.stack(arrived)
    feature_grad = jnp.concatenate(
        [
            lax.dynamic_index_in_dim(arrived, (row - j + fold) % fold, 0, keepdims=False)
            for j in range(fold)
        ],
        axis=1,
    ).astype(jnp.float32)
    slice_width = feature_grad.shape[1]
    col_start = lax.axis_index("col") * slice_width
    input_part = lax.dynamic_slice_in_dim(inputs, col_start, slice_width, 1)
    gain_part = lax.dynamic_slice_in_dim(gain, col_start, slice_width, 0)
    weighted = gain_part * feature_grad
    token_dot = lax.psum(jnp.sum(weighted * input_part, axis=1, keepdims=True), "col")
    d_input = (
        d_resid.astype(jnp.float32)
        + inv_rms * weighted
        - input_part * inv_rms**3 * token_dot / model_width
    ).astype(jnp.bfloat16)
    gain_partial = jnp.sum(feature_grad * input_part * inv_rms, axis=0) * scaling
    cotangent = jnp.concatenate([d_query, d_keyval], axis=1)
    columns = lax.all_to_all(normed, "row", split_axis=1, concat_axis=0, tiled=True)
    groups = lax.axis_size("row")
    column_blocks = columns.reshape(groups, local_tokens, columns.shape[1])
    grad_blocks = all_cotangents.reshape(groups, local_tokens, all_cotangents.shape[1])
    blocks = (
        lax.dot_general(
            column_blocks,
            grad_blocks,
            (((1,), (1,)), ((0,), (0,))),
            preferred_element_type=jnp.float32,
        )
        * weight_scale
    )
    summed = jnp.sum(blocks.astype(jnp.bfloat16).astype(jnp.float32), axis=0)
    grad_wq = summed[:, :query_cols].astype(jnp.bfloat16)
    grad_wkv = summed[:, query_cols:].astype(jnp.bfloat16)
    query_f = grad_wq.astype(jnp.float32)
    keyval_f = grad_wkv.astype(jnp.float32)
    tile_square = jnp.sum(query_f * query_f) + jnp.sum(keyval_f * keyval_f)
    grad_gain = lax.psum(gain_partial, "row")
    leading = jnp.where(
        lax.axis_index("row") == 0, jnp.sum(grad_gain * grad_gain), jnp.float32(0.0)
    )
    grand_total = lax.psum(tile_square + leading, ("row", "col"))
    grad_square_sum = grand_total / jnp.float32(model_width)
    return (d_input, grad_wq, grad_wkv, grad_gain, grad_square_sum)


def solution(mesh):
    placed = (
        P("row", None),
        P(),
        P("row", "col"),
        P("row", "col"),
        P("row", "col"),
        P("row", "col"),
        P("row", "col"),
    )
    return jax.shard_map(
        local,
        mesh=mesh,
        in_specs=placed,
        out_specs=(P("row", "col"), P("row", "col"), P("row", "col"), P("col"), P()),
        check_vma=False,
    )
```

```python
import functools
import math

import jax
import jax.numpy as jnp
from jax import lax
from jax.experimental import pallas as pl
from jax.experimental.pallas import tpu as pltpu
from jax.sharding import PartitionSpec as P

epsilon = 1e-05
MESH = pl.DeviceIdType.MESH
PIECES = 2


def ring_order(place, n):
    return jnp.where(place < n // 2, 2 * place, 2 * (n - 1 - place) + 1)


def ring_place(index, n):
    half = index // 2
    return jnp.where(index % 2 == 0, half, n - 1 - half)


def greet(row, col, n_row, n_col):
    barrier = pltpu.get_barrier_semaphore()
    for k in range(1, n_row):
        pl.semaphore_signal(
            barrier, inc=1, device_id=((row + k) % n_row, col), device_id_type=MESH
        )
    for k in range(1, n_col):
        pl.semaphore_signal(
            barrier, inc=1, device_id=(row, (col + k) % n_col), device_id_type=MESH
        )
    pl.semaphore_wait(barrier, n_row + n_col - 2)


def gather_kernel(
    n_row, n_col, cot, normed, all_cot, columns,
    own_sem, ring_send, ring_recv, swap_send, swap_recv, share_send, share_recv,
):
    row, col = lax.axis_index("row"), lax.axis_index("col")
    tokens = cot.shape[0]
    width = columns.shape[2]
    part = tokens // n_col
    piece = tokens // (2 * PIECES)
    place = ring_place(row, n_row)
    ahead = ring_order((place + 1) % n_row, n_row)
    behind = ring_order((place + n_row - 1) % n_row, n_row)
    greet(row, col, n_row, n_col)

    own_rows = pl.ds(pl.multiple_of(col * part, part), part)

    def ring_copy(step, way, q):
        if way == 0:
            source, target = ring_order((place + n_row - step) % n_row, n_row), ahead
        else:
            source, target = ring_order((place + step) % n_row, n_row), behind
        rows = pl.ds((way * PIECES + q) * piece, piece)
        return pltpu.make_async_remote_copy(
            src_ref=cot.at[rows] if step == 0 else all_cot.at[source, rows],
            dst_ref=all_cot.at[source, rows],
            send_sem=ring_send.at[step, way, q],
            recv_sem=ring_recv.at[step, way, q],
            device_id=(target, col),
            device_id_type=MESH,
        )

    def swap_copy(k):
        target = ring_order((place + k) % n_row, n_row)
        return pltpu.make_async_remote_copy(
            src_ref=normed.at[own_rows, pl.ds(pl.multiple_of(target * width, width), width)],
            dst_ref=columns.at[row, own_rows],
            send_sem=swap_send.at[k],
            recv_sem=swap_recv.at[k],
            device_id=(target, col),
            device_id_type=MESH,
        )

    own_columns = pl.ds(pl.multiple_of(row * width, width), width)

    def share_copy(k, j):
        source = ring_order((place + n_row - k) % n_row, n_row)
        return pltpu.make_async_remote_copy(
            src_ref=columns.at[source, own_rows],
            dst_ref=columns.at[source, own_rows],
            send_sem=share_send.at[k, j],
            recv_sem=share_recv.at[k, j],
            device_id=(row, (col + j) % n_col),
            device_id_type=MESH,
        )

    keep_cot = pltpu.make_async_copy(cot, all_cot.at[row], own_sem.at[0])
    keep_normed = pltpu.make_async_copy(
        normed.at[:, own_columns], columns.at[row], own_sem.at[1]
    )
    rings = {}
    swaps = {}
    shares = []
    for step in range(n_row):
        for q in range(PIECES):
            for way in range(2):
                if step > 0:
                    rings[step - 1, way, q].wait_recv()
                if step < n_row - 1:
                    rings[step, way, q] = ring_copy(step, way, q)
                    rings[step, way, q].start()
        if step == 0:
            keep_cot.start()
            keep_normed.start()
        if step < n_row - 1:
            swaps[step + 1] = swap_copy(step + 1)
            swaps[step + 1].start()
        if step > 0:
            swaps[step].wait_recv()
            for j in range(1, n_col):
                copy = share_copy(step, j)
                copy.start()
                shares.append(copy)
    keep_cot.wait()
    keep_normed.wait()
    for copy in list(rings.values()) + list(swaps.values()):
        copy.wait_send()
    for copy in shares:
        copy.wait()


def gather(cot, normed, n_row, n_col):
    tokens, cot_width = cot.shape
    width = normed.shape[1] // n_row
    dma = pltpu.SemaphoreType.DMA
    return pl.pallas_call(
        functools.partial(gather_kernel, n_row, n_col),
        out_shape=(
            jax.ShapeDtypeStruct((n_row, tokens, cot_width), cot.dtype),
            jax.ShapeDtypeStruct((n_row, tokens, width), normed.dtype),
        ),
        in_specs=[pl.BlockSpec(memory_space=pltpu.VMEM)] * 2,
        out_specs=[pl.BlockSpec(memory_space=pl.ANY)] * 2,
        scratch_shapes=[
            dma((2,)),
            dma((n_row, 2, PIECES)),
            dma((n_row, 2, PIECES)),
            dma((n_row,)),
            dma((n_row,)),
            dma((n_row, n_col)),
            dma((n_row, n_col)),
        ],
        compiler_params=pltpu.CompilerParams(collective_id=0, has_side_effects=True),
        name="gather",
    )(cot, normed)


def sums_kernel(
    n_row, n_col, dots, gains, dots_out, gains_out,
    dots_in, gains_in, dots_send, dots_recv, gains_send, gains_recv,
):
    row, col = lax.axis_index("row"), lax.axis_index("col")
    greet(row, col, n_row, n_col)
    copies = []
    for k in range(1, n_col):
        copies.append(
            pltpu.make_async_remote_copy(
                src_ref=dots,
                dst_ref=dots_in.at[col],
                send_sem=dots_send.at[k],
                recv_sem=dots_recv.at[k],
                device_id=(row, (col + k) % n_col),
                device_id_type=MESH,
            )
        )
    for k in range(1, n_row):
        copies.append(
            pltpu.make_async_remote_copy(
                src_ref=gains,
                dst_ref=gains_in.at[row],
                send_sem=gains_send.at[k],
                recv_sem=gains_recv.at[k],
                device_id=((row + k) % n_row, col),
                device_id_type=MESH,
            )
        )
    for copy in copies:
        copy.start()
    dots_in[col] = dots[...]
    gains_in[row] = gains[...]
    for copy in copies:
        copy.wait()
    dots_out[...] = jnp.sum(dots_in[...], axis=0)
    gains_out[...] = jnp.sum(gains_in[...], axis=0)


def sums(dots, gains, n_row, n_col):
    dma = pltpu.SemaphoreType.DMA
    return pl.pallas_call(
        functools.partial(sums_kernel, n_row, n_col),
        out_shape=(
            jax.ShapeDtypeStruct(dots.shape, dots.dtype),
            jax.ShapeDtypeStruct(gains.shape, gains.dtype),
        ),
        in_specs=[pl.BlockSpec(memory_space=pltpu.VMEM)] * 2,
        out_specs=[pl.BlockSpec(memory_space=pltpu.VMEM)] * 2,
        scratch_shapes=[
            pltpu.VMEM((n_col,) + dots.shape, dots.dtype),
            pltpu.VMEM((n_row,) + gains.shape, gains.dtype),
            dma((n_col,)),
            dma((n_col,)),
            dma((n_row,)),
            dma((n_row,)),
        ],
        compiler_params=pltpu.CompilerParams(collective_id=1, has_side_effects=True),
        name="sums",
    )(dots, gains)


def local(layer_input, gain, d_query, d_keyval, w_query, w_keyval, d_resid):
    inputs = layer_input.astype(jnp.float32)
    inv_rms = lax.rsqrt(jnp.mean(inputs * inputs, axis=1, keepdims=True) + epsilon)
    normed = (inputs * inv_rms * gain).astype(jnp.bfloat16)
    model_width = inputs.shape[1]
    local_tokens = inputs.shape[0]
    tokens_all = local_tokens * lax.axis_size("row")
    scaling = 1.0 / math.sqrt(tokens_all)
    weight_scale = 1.0 / math.sqrt(local_tokens)
    contract_cols = (((1,), (1,)), ((), ()))
    query_cols = d_query.shape[1]
    cotangent = jnp.concatenate([d_query, d_keyval], axis=1)
    n_row, n_col = lax.axis_size("row"), lax.axis_size("col")
    all_cotangents, columns = gather(cotangent, normed, n_row, n_col)
    all_cotangents = all_cotangents.reshape(-1, cotangent.shape[1])
    columns = columns.reshape(all_cotangents.shape[0], -1)
    weights = jnp.concatenate([w_query, w_keyval], axis=1)
    partial_value = lax.dot_general(
        all_cotangents, weights, contract_cols, preferred_element_type=jnp.float32
    )
    reduced = lax.psum_scatter(
        partial_value.astype(jnp.bfloat16), "col", scatter_dimension=0, tiled=True
    )
    fold = n_row // n_col
    pieces = reduced.reshape(fold, local_tokens, reduced.shape[1])
    row, col = lax.axis_index("row"), lax.axis_index("col")
    arrived = []
    for shift in range(fold):
        pairs = [
            (r * n_col + c, (fold * c + (r + shift) % fold) * n_col + r // fold)
            for r in range(n_row)
            for c in range(n_col)
        ]
        piece = lax.dynamic_index_in_dim(pieces, (row + shift) % fold, 0, keepdims=False)
        arrived.append(lax.ppermute(piece, ("row", "col"), pairs))
    arrived = jnp.stack(arrived)
    feature_grad = jnp.concatenate(
        [
            lax.dynamic_index_in_dim(arrived, (row - j + fold) % fold, 0, keepdims=False)
            for j in range(fold)
        ],
        axis=1,
    ).astype(jnp.float32)
    slice_width = feature_grad.shape[1]
    col_start = lax.axis_index("col") * slice_width
    input_part = lax.dynamic_slice_in_dim(inputs, col_start, slice_width, 1)
    gain_part = lax.dynamic_slice_in_dim(gain, col_start, slice_width, 0)
    weighted = gain_part * feature_grad
    gain_partial = jnp.sum(feature_grad * input_part * inv_rms, axis=0) * scaling
    dots, gains = sums(
        jnp.sum(weighted * input_part, axis=1).reshape(-1, 128),
        gain_partial.reshape(-1, 128),
        n_row,
        n_col,
    )
    token_dot = dots.reshape(local_tokens, 1)
    grad_gain = gains.reshape(slice_width)
    d_input = (
        d_resid.astype(jnp.float32)
        + inv_rms * weighted
        - input_part * inv_rms**3 * token_dot / model_width
    ).astype(jnp.bfloat16)
    summed = (
        lax.dot_general(
            columns, all_cotangents, (((0,), (0,)), ((), ())), preferred_element_type=jnp.float32
        )
        * weight_scale
    )
    grad_wq = summed[:, :query_cols].astype(jnp.bfloat16)
    grad_wkv = summed[:, query_cols:].astype(jnp.bfloat16)
    query_f = grad_wq.astype(jnp.float32)
    keyval_f = grad_wkv.astype(jnp.float32)
    tile_square = jnp.sum(query_f * query_f) + jnp.sum(keyval_f * keyval_f)
    leading = jnp.where(
        lax.axis_index("row") == 0, jnp.sum(grad_gain * grad_gain), jnp.float32(0.0)
    )
    grand_total = lax.psum(tile_square + leading, ("row", "col"))
    grad_square_sum = grand_total / jnp.float32(model_width)
    return (d_input, grad_wq, grad_wkv, grad_gain, grad_square_sum)


def solution(mesh):
    placed = (
        P("row", None),
        P(),
        P("row", "col"),
        P("row", "col"),
        P("row", "col"),
        P("row", "col"),
        P("row", "col"),
    )
    return jax.shard_map(
        local,
        mesh=mesh,
        in_specs=placed,
        out_specs=(P("row", "col"), P("row", "col"), P("row", "col"), P("col"), P()),
        check_vma=False,
    )
```
